32 devices in a mesh: dp: 8 (over y, x, core), shard: 4 (over z).
Axes of the slice: x: 2, y: 2, z: 4, core: 2. Of those that a mesh axis runs over, the one named last changes fastest.
Arguments:
- tokens: bfloat16 [4096, 800], P(('dp', 'shard')), may hold values from -6 to 6
- cotangent: bfloat16 [4096, 800], P(('dp', 'shard')), may hold values from -6 to 6
- lengths: int32 [32, 1], P(('dp', 'shard')), may hold values from 0 to 128, as said below
- master: float32 [12746752], P('shard'), may hold values from -6 to 6
- moment_first: float32 [12746752], P('shard'), may hold values from -0.0029296875 to 0.0029296875
- moment_second: float32 [12746752], P('shard'), may hold values from 1e-09 to 1e-08
Outputs:
- block_output: bfloat16 [4096, 800], P(('dp', 'shard'))
- token_grad: bfloat16 [4096, 800], P(('dp', 'shard'))
- weight_grad: float32 [12746752], P('shard')
- new_master: float32 [12746752], P('shard')
- new_moment_first: float32 [12746752], P('shard')
- new_moment_second: float32 [12746752], P('shard')
The draws below stay inside these ranges and needn't reach their ends.
Inputs may be any that keep to these rules, and one draw needn't show every extreme that they name: `lengths`: each device's sequences come first and are followed by zeros; together they take at most 1 block of 128; every device has a sequence; some device holds one sequence of 128 tokens.
All inputs are finite; a program needn't handle non-finite values.
Results may differ from the reference program's by a relative error of at most 0.01.
The reference program's roundings to bfloat16 on the way (of `weights`, `normed`, `probs_low`, `heads_out`, `activated`, `gated_out`, `normed_ffn` and `swished`) count: a program that leaves them out, or rounds other values in their place, can miss the bound.
Values may be sent and summed in bfloat16 or wider, within the bound.
A program may use at most 384 MiB of HBM per device.

```python
import math
from functools import partial
import jax
import jax.numpy as jnp
from jax import lax

D = 800
HEADS = 15
KVH = 5
HEAD = 64
INNER = 1600
STATE = 16
DTR = 50
CONV = 4
FF = 2752
BLOCK = 128
TOK_DEV = 128
SEQS = 1
ROWS = 4096
PARAMS = 12744000
PTOT = 12746752
DEVICES = 32


def draw_lengths(key, part):
    device_ids = jnp.arange(DEVICES, dtype=jnp.int32)[:, None]
    block_ids = jnp.arange(SEQS, dtype=jnp.int32)[None, :]
    live_blocks = 1 + (SEQS - 1) * device_ids // max(DEVICES - 1, 1)
    final_device = device_ids == DEVICES - 1
    cut_flags = jax.random.randint(jax.random.fold_in(key, 3), (DEVICES, SEQS), 0, 2)
    in_use = block_ids < live_blocks
    begins = ((block_ids == 0) | (cut_flags == 1) & jnp.logical_not(final_device)) & in_use
    sequence_of = jnp.cumsum(begins.astype(jnp.int32), axis=1) - 1
    slot_ids = jnp.arange(SEQS, dtype=jnp.int32)
    member = ((sequence_of[:, None, :] == slot_ids[None, :, None]) & in_use[:, None, :]).astype(jnp.int32)
    block_counts = jnp.sum(member, axis=2)
    tail_sizes = jax.random.randint(jax.random.fold_in(key, 5), (DEVICES, SEQS), 1, BLOCK + 1)
    tail_sizes = jnp.where(final_device, BLOCK, tail_sizes)
    lengths = jnp.where(block_counts > 0, BLOCK * block_counts - BLOCK + tail_sizes, 0)
    return lengths.astype(jnp.int32)


def draw_master(key, part):
    mixing = HEADS * HEAD + 2 * KVH * HEAD + 2 * INNER
    sections = [(D, 1.0, 0.25), (D * mixing, 0.0, D ** (-0.5)), (HEADS * HEAD * D, 0.0, (HEADS * HEAD) ** (-0.5)), (CONV * INNER, 0.0, 0.5), (INNER, 0.0, 0.3), (INNER * (DTR + 2 * STATE), 0.0, INNER ** (-0.5)), (DTR * INNER, 0.0, 0.5 * DTR ** (-0.5)), (INNER, -3.2, 0.5), (STATE * INNER, 1.4, 0.5), (INNER, 1.0, 0.3), (INNER * D, 0.0, INNER ** (-0.5)), (D, 1.0, 0.25), (D, 1.0, 0.25), (D, 1.0, 0.25), (2 * D * FF, 0.0, D ** (-0.5)), (FF * D, 0.0, FF ** (-0.5))]
    pieces = []
    for position, (amount, centre, spread) in enumerate(sections):
        sub_key = jax.random.fold_in(key, 17 + position)
        noise_vals = jnp.clip(jax.random.normal(sub_key, (amount,), jnp.float32), -4.0, 4.0)
        pieces.append(centre + spread * noise_vals)
    padding = 0.02 * jnp.clip(jax.random.normal(jax.random.fold_in(key, 99), (PTOT - PARAMS,), jnp.float32), -4.0, 4.0)
    return jnp.concatenate(pieces + [padding])


def level_of(stream_key, extent, cuts, least, high):
    level, own = 1.0, jax.random.fold_in(stream_key, 6)
    for axis_at, blocks in cuts:
        draws = jnp.exp(jax.random.uniform(jax.random.fold_in(own, axis_at), (blocks,), jnp.float32, least / len(cuts), high / len(cuts)))
        level = level * jnp.repeat(draws, extent[axis_at] // blocks).reshape([-1 if axis == axis_at else 1 for axis in range(len(extent))])
    return level


def normal_values(stream_key, dims, scale, bound, shards=(), held_as=jnp.bfloat16):
    result = scale * jax.random.normal(stream_key, dims, jnp.float32)
    if shards:
        result = result * level_of(stream_key, dims, shards, -0.22, 0.18)
    return jnp.clip(result, -bound, bound).astype(held_as)


def setup_inputs(seed: int = 0) -> dict:
    keys = jax.random.split(jax.random.key(seed), 7)
    return {
        "tokens": normal_values(keys[0], (ROWS, D), 1.0, 6.0, ((0, 32),)),
        "cotangent": normal_values(keys[1], (ROWS, D), 1.0, 6.0, ((0, 32),)),
        "lengths": draw_lengths(jax.random.fold_in(keys[6], 71), 0),
        "master": draw_master(jax.random.fold_in(keys[6], 71), 0),
        "moment_first": normal_values(keys[4], (PTOT,), 0.0002, 0.0029296875, ((0, 4),), jnp.float32),
        "moment_second": jnp.clip(jnp.exp(math.log(9.99999993922529e-09) - 2.3025851 * jax.random.uniform(keys[5], (PTOT,), jnp.float32) ** level_of(keys[5], (PTOT,), ((0, 4),), -0.2, 0.2)), 9.999999717180685e-10, 9.99999993922529e-09),
    }


EPS = 1e-05
LEARN = 0.03
BETA_FIRST = 0.9
BETA_SECOND = 0.999
FIX_FIRST = 1.0 - 0.9 ** 3
FIX_SECOND = 1.0 - 0.999 ** 3
DECAY = 0.1
ADAM_EPS = 1e-08
NEGATIVE = -1e+30

def matmul_f32(left, right):
    return jnp.dot(left, right, preferred_element_type=jnp.float32)

def batched(formula, left, right):
    return jnp.einsum(formula, left.astype(jnp.float32), right.astype(jnp.float32))

def param_shapes():
    mixing = HEADS * HEAD + 2 * KVH * HEAD + 2 * INNER
    return [(D,), (D, mixing), (HEADS * HEAD, D), (CONV, INNER), (INNER,), (INNER, DTR + 2 * STATE), (DTR, INNER), (INNER,), (STATE, INNER), (INNER,), (INNER, D), (D,), (D,), (D,), (D, 2 * FF), (FF, D)]

def unpack(flat_params):
    pieces = []
    cursor = 0
    for layout_shape in param_shapes():
        amount = math.prod(layout_shape)
        pieces.append(flat_params[cursor:cursor + amount].reshape(layout_shape))
        cursor += amount
    return pieces

def rms_norm(values, scale_gain):
    return values * lax.rsqrt(lax.optimization_barrier(jnp.mean(values * values, axis=-1, keepdims=True)) + EPS) * scale_gain

def token_layout(lengths, row_total):
    lengths = lengths.astype(jnp.int32)
    seq_slots = lengths.shape[0]
    blocks_used = ((lengths + BLOCK - 1) // BLOCK).astype(jnp.int32)
    firsts = (jnp.cumsum(blocks_used) - blocks_used).astype(jnp.int32)
    block_ids = jnp.arange(seq_slots, dtype=jnp.int32)
    inside = ((block_ids[:, None] >= firsts[None, :]) & (block_ids[:, None] < (firsts + blocks_used)[None, :])).astype(jnp.int32)
    occupied = lax.optimization_barrier(jnp.sum(inside, axis=1)) > 0
    block_segment = jnp.where(occupied, lax.optimization_barrier(jnp.sum(inside * block_ids[None, :], axis=1)).astype(jnp.int32), seq_slots + block_ids)
    block_begin = jnp.where(occupied, lax.optimization_barrier(jnp.sum(inside * firsts[None, :], axis=1)).astype(jnp.int32), block_ids)
    block_length = lax.optimization_barrier(jnp.sum(inside * lengths[None, :], axis=1)).astype(jnp.int32)
    rows_index = jnp.arange(row_total, dtype=jnp.int32)
    owner_block = (rows_index[:, None] // BLOCK == block_ids[None, :]).astype(jnp.int32)
    segment = lax.optimization_barrier(jnp.sum(owner_block * block_segment[None, :], axis=1)).astype(jnp.int32)
    places = (rows_index - BLOCK * lax.optimization_barrier(jnp.sum(owner_block * block_begin[None, :], axis=1))).astype(jnp.int32)
    live_rows = places < lax.optimization_barrier(jnp.sum(owner_block * block_length[None, :], axis=1)).astype(jnp.int32)
    return (segment, places, live_rows)

def conv_silu(inner_in, conv_weight, conv_bias, places):
    summed = conv_bias + conv_weight[CONV - 1] * inner_in
    for offset in range(1, CONV):
        shifted = jnp.concatenate([jnp.zeros((offset, inner_in.shape[1]), inner_in.dtype), inner_in[:-offset]], axis=0)
        summed = summed + conv_weight[CONV - 1 - offset] * jnp.where((places >= offset)[:, None], shifted, jnp.zeros_like(shifted))
    return jax.nn.silu(summed)

def selective_scan(steps_dt, inputs, b_rows, c_rows, decay_log, fresh_rows):
    decay_rates = -jnp.exp(decay_log)

    def advance(carried, step_items):
        step_dt, step_in, step_b, step_c, step_fresh = step_items
        carried = jnp.exp(step_dt[None, :] * decay_rates) * carried * (1.0 - step_fresh) + step_b[:, None] * (step_dt * step_in)[None, :]
        return (carried, lax.optimization_barrier(jnp.sum(step_c[:, None] * carried, axis=0)))

    def run_block(carried, step_items):
        return lax.scan(advance, carried, step_items)
    run_block = jax.checkpoint(run_block)
    row_total = inputs.shape[0]
    blocks = row_total // BLOCK
    shaped = tuple((member.reshape((blocks, BLOCK) + member.shape[1:]) for member in (steps_dt, inputs, b_rows, c_rows, fresh_rows)))
    start_state = jnp.zeros((decay_log.shape[0], inputs.shape[1]), inputs.dtype)
    _, outputs = lax.scan(run_block, start_state, shaped)
    return outputs.reshape(row_total, inputs.shape[1])

def mamba_tail(dt_raw, dt_bias, inputs, b_rows, c_rows, decay_log, skip, z_gate, fresh_rows):
    steps_dt = jax.nn.softplus(dt_raw + dt_bias)
    scanned = selective_scan(steps_dt, inputs, b_rows, c_rows, decay_log, fresh_rows)
    return (scanned + skip * inputs) * jax.nn.silu(z_gate)

def merge_branches(attn_out, ssm_out, beta_attn, beta_ssm):
    return 0.5 * (rms_norm(attn_out, beta_attn) + rms_norm(ssm_out, beta_ssm))

def swiglu(gate_up):
    return jax.nn.silu(gate_up[:, :FF]) * gate_up[:, FF:]

def attention_scores(query_rows, key_rows, allowed):
    row_total = query_rows.shape[0]
    query_heads = query_rows.reshape(row_total, KVH, HEADS // KVH, HEAD)
    key_heads = key_rows.reshape(row_total, KVH, HEAD)
    scores = batched('qkgd,pkd->kgqp', query_heads, key_heads) * HEAD ** (-0.5)
    return jnp.where(allowed, scores, NEGATIVE)

def attend_back(query_rows, key_rows, value_rows, soft_probs, d_heads):
    row_total = query_rows.shape[0]
    group_size = HEADS // KVH
    query_heads = query_rows.reshape(row_total, KVH, group_size, HEAD)
    key_heads = key_rows.reshape(row_total, KVH, HEAD)
    value_heads = value_rows.reshape(row_total, KVH, HEAD)
    probs_low = soft_probs.astype(jnp.bfloat16)
    d_heads4 = d_heads.reshape(row_total, KVH, group_size, HEAD)
    d_values = batched('kgqp,qkgd->pkd', probs_low, d_heads4)
    d_probs = batched('qkgd,pkd->kgqp', d_heads4, value_heads)
    centre = lax.optimization_barrier(jnp.sum(soft_probs * d_probs, axis=-1, keepdims=True))
    d_scores = (soft_probs * (d_probs - centre) * HEAD ** (-0.5)).astype(jnp.bfloat16)
    d_query = batched('kgqp,pkd->qkgd', d_scores, key_heads)
    d_keys = batched('kgqp,qkgd->pkd', d_scores, query_heads)
    return (d_query.reshape(row_total, HEADS * HEAD), d_keys.reshape(row_total, KVH * HEAD), d_values.reshape(row_total, KVH * HEAD))

def layer_pass(params, tokens, cotangent, lengths):
    gain_in, w_mixing, w_attn, conv_weight, conv_bias, w_project, w_dt, dt_bias, decay_log, skip, w_ssm, beta_attn, beta_ssm, gain_ffn, w_gate_up, w_down = unpack(params)
    wide = jnp.float32
    row_total = tokens.shape[0]
    segment, places, live_rows = token_layout(lengths, row_total)
    fresh_rows = (places == 0).astype(wide)
    allowed = (segment[:, None] == segment[None, :]) & (places[None, :] <= places[:, None])
    residual = tokens.astype(wide)
    normed, norm_back = jax.vjp(rms_norm, residual, gain_in.astype(wide))
    normed_low = normed.astype(jnp.bfloat16)
    mixing = matmul_f32(normed_low, w_mixing)
    width_q = HEADS * HEAD
    width_kv = KVH * HEAD
    query_rows = mixing[:, :width_q].astype(jnp.bfloat16)
    key_rows = mixing[:, width_q:width_q + width_kv].astype(jnp.bfloat16)
    value_rows = mixing[:, width_q + width_kv:width_q + 2 * width_kv].astype(jnp.bfloat16)
    inner_in = mixing[:, width_q + 2 * width_kv:width_q + 2 * width_kv + INNER]
    z_gate = mixing[:, width_q + 2 * width_kv + INNER:]
    scores = attention_scores(query_rows, key_rows, allowed)
    row_max = lax.optimization_barrier(jnp.max(scores, axis=-1, keepdims=True))
    logsum = row_max + jnp.log(lax.optimization_barrier(jnp.sum(jnp.exp(scores - row_max), axis=-1, keepdims=True)))
    probs_low = jnp.exp(scores - logsum).astype(jnp.bfloat16)
    value_heads = value_rows.reshape(row_total, KVH, HEAD)
    heads_out = batched('kgqp,pkd->qkgd', probs_low, value_heads).reshape(row_total, width_q).astype(jnp.bfloat16)
    attn_out = matmul_f32(heads_out, w_attn)
    activated, conv_back = jax.vjp(partial(conv_silu, places=places), inner_in, conv_weight.astype(wide), conv_bias.astype(wide))
    activated_low = activated.astype(jnp.bfloat16)
    projected = matmul_f32(activated_low, w_project)
    dt_low = projected[:, :DTR].astype(jnp.bfloat16)
    b_rows = projected[:, DTR:DTR + STATE]
    c_rows = projected[:, DTR + STATE:]
    dt_raw = matmul_f32(dt_low, w_dt)
    activated_wide = lax.optimization_barrier(activated_low).astype(wide)
    gated_out, tail_back = jax.vjp(partial(mamba_tail, fresh_rows=fresh_rows), dt_raw, dt_bias.astype(wide), activated_wide, b_rows, c_rows, decay_log.astype(wide), skip.astype(wide), z_gate)
    gated_low = gated_out.astype(jnp.bfloat16)
    ssm_out = matmul_f32(gated_low, w_ssm)
    branch_mix, merge_back = jax.vjp(merge_branches, attn_out, ssm_out, beta_attn.astype(wide), beta_ssm.astype(wide))
    hidden = residual + branch_mix
    normed_ffn, ffn_norm_back = jax.vjp(rms_norm, hidden, gain_ffn.astype(wide))
    normed_ffn_low = normed_ffn.astype(jnp.bfloat16)
    gate_up = matmul_f32(normed_ffn_low, w_gate_up)
    swished, swiglu_back = jax.vjp(swiglu, gate_up)
    swished_low = swished.astype(jnp.bfloat16)
    output = hidden + matmul_f32(swished_low, w_down)
    d_out = jnp.where(live_rows[:, None], cotangent, jnp.zeros_like(cotangent))
    grad_down = matmul_f32(swished_low.T, d_out)
    d_gate_up, = swiglu_back(matmul_f32(d_out, w_down.T))
    d_gate_up_low = d_gate_up.astype(jnp.bfloat16)
    grad_gate_up = matmul_f32(normed_ffn_low.T, d_gate_up_low)
    d_hidden, grad_gain_ffn = ffn_norm_back(matmul_f32(d_gate_up_low, w_gate_up.T))
    d_hidden = d_hidden + d_out.astype(wide)
    d_attn, d_ssm, grad_beta_attn, grad_beta_ssm = merge_back(d_hidden)
    d_ssm_low = d_ssm.astype(jnp.bfloat16)
    grad_ssm = matmul_f32(gated_low.T, d_ssm_low)
    d_dt_raw, grad_dt_bias, d_activated, d_b_rows, d_c_rows, grad_decay, grad_skip, d_z_gate = tail_back(matmul_f32(d_ssm_low, w_ssm.T))
    d_dt_low = d_dt_raw.astype(jnp.bfloat16)
    grad_dt = matmul_f32(dt_low.T, d_dt_low)
    d_projected = jnp.concatenate([matmul_f32(d_dt_low, w_dt.T), d_b_rows, d_c_rows], axis=1).astype(jnp.bfloat16)
    grad_project = matmul_f32(activated_low.T, d_projected)
    d_activated = d_activated + matmul_f32(d_projected, w_project.T)
    d_inner_in, grad_conv_weight, grad_conv_bias = conv_back(d_activated)
    d_attn_low = d_attn.astype(jnp.bfloat16)
    grad_attn = matmul_f32(heads_out.T, d_attn_low)
    d_heads = matmul_f32(d_attn_low, w_attn.T).astype(jnp.bfloat16)
    soft_probs = jnp.exp(attention_scores(query_rows, key_rows, allowed) - logsum)
    d_query, d_keys, d_values = attend_back(query_rows, key_rows, value_rows, soft_probs, d_heads)
    d_mixing = jnp.concatenate([d_query, d_keys, d_values, d_inner_in, d_z_gate], axis=1).astype(jnp.bfloat16)
    grad_mixing = matmul_f32(normed_low.T, d_mixing)
    d_residual, grad_gain_in = norm_back(matmul_f32(d_mixing, w_mixing.T))
    d_tokens = d_hidden + d_residual
    gradients = [grad_gain_in, grad_mixing, grad_attn, grad_conv_weight, grad_conv_bias, grad_project, grad_dt, grad_dt_bias, grad_decay, grad_skip, grad_ssm, grad_beta_attn, grad_beta_ssm, grad_gain_ffn, grad_gate_up, grad_down]
    flat_grad = jnp.concatenate([member.reshape(-1) for member in gradients] + [jnp.zeros((params.shape[0] - PARAMS,), wide)])
    live_count = jnp.sum(live_rows.astype(wide))
    return (output.astype(jnp.bfloat16), d_tokens, flat_grad, live_count)

def adamw_update(weight, gradient, first_moment, second):
    first_moment = BETA_FIRST * first_moment + (1.0 - BETA_FIRST) * gradient
    second = BETA_SECOND * second + (1.0 - BETA_SECOND) * gradient * gradient
    step_size = first_moment / FIX_FIRST / (jnp.sqrt(second / FIX_SECOND) + ADAM_EPS)
    return (weight - LEARN * (step_size + DECAY * weight), first_moment, second)

def reference(tokens, cotangent, lengths, master, moment_first, moment_second):
    weights = master.astype(jnp.bfloat16)
    device_total = lengths.shape[0]

    def one_device(carried, step_items):
        summed, counted = carried
        token_block, cot_block, length_row = step_items
        output, d_tokens, flat_grad, live_count = layer_pass(weights, token_block, cot_block, length_row)
        return ((summed + flat_grad, counted + live_count), (output, d_tokens.astype(jnp.bfloat16)))
    initial = (jnp.zeros((PTOT,), jnp.float32), jnp.zeros((), jnp.float32))
    stacked = (tokens.reshape(device_total, TOK_DEV, D), cotangent.reshape(device_total, TOK_DEV, D), lengths)
    (summed, counted), (outputs, d_tokens) = lax.scan(one_device, initial, stacked)
    gradient = summed / counted
    new_master, new_first, new_second = adamw_update(master, gradient, moment_first, moment_second)
    return (outputs.reshape(ROWS, D), d_tokens.reshape(ROWS, D), gradient, new_master, new_first, new_second)
```

```python
from functools import partial
import math

import jax
import jax.numpy as jnp
from jax import lax
from jax.experimental import pallas as pl
from jax.experimental.pallas import tpu as pltpu
from jax.sharding import PartitionSpec as P

D = 800
HEADS = 15
KVH = 5
HEAD = 64
INNER = 1600
STATE = 16
DTR = 50
CONV = 4
FF = 2752
BLOCK = 128
PARAMS = 12744000


LANES = 128
SUBS = 16
ROWS_STEP = 16


def spread_rows(source, target):
    rows = source.shape[0]
    for base in range(0, rows, 8):
        for chunk in range(SUBS):
            target[pl.ds(base * SUBS + chunk, 8, stride=SUBS), :] = source[
                base : base + 8, chunk * LANES : (chunk + 1) * LANES
            ]


def gather_rows(source, target):
    rows = target.shape[0]
    for base in range(0, rows, 8):
        for chunk in range(SUBS):
            target[base : base + 8, chunk * LANES : (chunk + 1) * LANES] = source[
                pl.ds(base * SUBS + chunk, 8, stride=SUBS), :
            ]


def scan_forward_kernel(
    b_ref, c_ref, dt_ref, in_ref, rate_ref, out_ref, past_ref, dt_rows, in_rows, out_rows, state
):
    states = rate_ref.shape[0]

    @pl.when(pl.program_id(0) == 0)
    def _():
        state[...] = jnp.zeros_like(state)

    spread_rows(dt_ref, dt_rows)
    spread_rows(in_ref, in_rows)
    first = pl.program_id(0) * ROWS_STEP

    def advance(row, carried):
        step_dt = dt_rows[pl.ds(row * SUBS, SUBS), :]
        step_in = step_dt * in_rows[pl.ds(row * SUBS, SUBS), :]
        total = jnp.zeros_like(step_dt)
        following = []
        for n in range(states):
            past_ref[row, n] = carried[n]
            fresh = jnp.exp(step_dt * rate_ref[n]) * carried[n] + b_ref[first + row, n] * step_in
            total = total + c_ref[first + row, n] * fresh
            following.append(fresh)
        out_rows[pl.ds(row * SUBS, SUBS), :] = total
        return tuple(following)

    carried = tuple(state[n] for n in range(states))
    carried = lax.fori_loop(0, ROWS_STEP, advance, carried)
    for n in range(states):
        state[n] = carried[n]
    gather_rows(out_rows, out_ref)


def scan_backward_kernel(
    b_ref,
    c_ref,
    dt_ref,
    in_ref,
    dy_ref,
    rate_ref,
    past_ref,
    d_dt_ref,
    d_in_ref,
    d_b_ref,
    d_c_ref,
    d_rate_ref,
    dt_rows,
    in_rows,
    dy_rows,
    d_dt_rows,
    d_in_rows,
    b_parts,
    c_parts,
    state,
):
    states = rate_ref.shape[0]
    steps = pl.num_programs(0)

    @pl.when(pl.program_id(0) == 0)
    def _():
        state[...] = jnp.zeros_like(state)
        d_rate_ref[...] = jnp.zeros_like(d_rate_ref)

    spread_rows(dt_ref, dt_rows)
    spread_rows(in_ref, in_rows)
    spread_rows(dy_ref, dy_rows)
    first = (steps - 1 - pl.program_id(0)) * ROWS_STEP

    def retreat(index, carried):
        row = ROWS_STEP - 1 - index
        step_dt = dt_rows[pl.ds(row * SUBS, SUBS), :]
        step_u = in_rows[pl.ds(row * SUBS, SUBS), :]
        step_dy = dy_rows[pl.ds(row * SUBS, SUBS), :]
        step_in = step_dt * step_u
        d_step = jnp.zeros_like(step_dt)
        d_dt = jnp.zeros_like(step_dt)
        earlier = []
        for n in range(states):
            rate = rate_ref[n]
            step_b = b_ref[first + row, n]
            decayed = jnp.exp(step_dt * rate)
            kept = decayed * past_ref[row, n]
            grad = carried[n] + c_ref[first + row, n] * step_dy
            now_state = kept + step_b * step_in
            part_c = step_dy * now_state
            part_b = grad * step_in
            c_parts[pl.ds(row * states * 8 + n * 8, 8), :] = part_c[:8] + part_c[8:]
            b_parts[pl.ds(row * states * 8 + n * 8, 8), :] = part_b[:8] + part_b[8:]
            d_step = d_step + step_b * grad
            turned = grad * kept
            d_dt = d_dt + turned * rate
            d_rate_ref[n] = d_rate_ref[n] + turned * step_dt
            earlier.append(grad * decayed)
        d_dt_rows[pl.ds(row * SUBS, SUBS), :] = d_dt + d_step * step_u
        d_in_rows[pl.ds(row * SUBS, SUBS), :] = d_step * step_dt
        return tuple(earlier)

    carried = tuple(state[n] for n in range(states))
    carried = lax.fori_loop(0, ROWS_STEP, retreat, carried)
    for n in range(states):
        state[n] = carried[n]
    gather_rows(d_dt_rows, d_dt_ref)
    gather_rows(d_in_rows, d_in_ref)
    for parts, sums in ((b_parts, d_b_ref), (c_parts, d_c_ref)):
        for row in range(ROWS_STEP):
            total = parts[pl.ds(row * states * 8, states, stride=8), :]
            for sub in range(1, 8):
                total = total + parts[pl.ds(row * states * 8 + sub, states, stride=8), :]
            sums[row * states : (row + 1) * states, :] = total


def scan_specs(states, width):
    return dict(
        scalars=pl.BlockSpec(memory_space=pltpu.SMEM),
        rate=pl.BlockSpec((states, SUBS, LANES), lambda i: (0, 0, 0)),
    )


def widen(values):
    width = SUBS * LANES
    return jnp.pad(values, ((0, 0), (0, width - values.shape[1])))


def scan_forward(steps_dt, inputs, b_rows, c_rows, rates):
    rows, inner = inputs.shape
    states = rates.shape[0]
    width = SUBS * LANES
    steps = rows // ROWS_STEP
    specs = scan_specs(states, width)
    wide_block = pl.BlockSpec((ROWS_STEP, width), lambda i: (i, 0))
    out, past = pl.pallas_call(
        scan_forward_kernel,
        name="scan_forward",
        grid=(steps,),
        out_shape=(
            jax.ShapeDtypeStruct((rows, width), jnp.float32),
            jax.ShapeDtypeStruct((rows, states, SUBS, LANES), jnp.float32),
        ),
        in_specs=[specs["scalars"], specs["scalars"], wide_block, wide_block, specs["rate"]],
        out_specs=(
            wide_block,
            pl.BlockSpec((ROWS_STEP, states, SUBS, LANES), lambda i: (i, 0, 0, 0)),
        ),
        scratch_shapes=[
            pltpu.VMEM((ROWS_STEP * SUBS, LANES), jnp.float32),
            pltpu.VMEM((ROWS_STEP * SUBS, LANES), jnp.float32),
            pltpu.VMEM((ROWS_STEP * SUBS, LANES), jnp.float32),
            pltpu.VMEM((states, SUBS, LANES), jnp.float32),
        ],
        cost_estimate=pl.CostEstimate(
            flops=7 * rows * states * width,
            transcendentals=rows * states * width,
            bytes_accessed=4 * rows * width * (states + 3),
        ),
    )(b_rows, c_rows, widen(steps_dt), widen(inputs), widen(rates).reshape(states, SUBS, LANES))
    return out[:, :inner], past


def scan_backward(steps_dt, inputs, b_rows, c_rows, rates, past, d_out):
    rows, inner = inputs.shape
    states = rates.shape[0]
    width = SUBS * LANES
    steps = rows // ROWS_STEP
    specs = scan_specs(states, width)
    wide_block = pl.BlockSpec((ROWS_STEP, width), lambda i: (steps - 1 - i, 0))
    pair_block = pl.BlockSpec((ROWS_STEP * states, LANES), lambda i: (steps - 1 - i, 0))
    row_buffer = pltpu.VMEM((ROWS_STEP * SUBS, LANES), jnp.float32)
    d_dt, d_in, d_b, d_c, d_rate = pl.pallas_call(
        scan_backward_kernel,
        name="scan_backward",
        grid=(steps,),
        out_shape=(
            jax.ShapeDtypeStruct((rows, width), jnp.float32),
            jax.ShapeDtypeStruct((rows, width), jnp.float32),
            jax.ShapeDtypeStruct((rows * states, LANES), jnp.float32),
            jax.ShapeDtypeStruct((rows * states, LANES), jnp.float32),
            jax.ShapeDtypeStruct((states, SUBS, LANES), jnp.float32),
        ),
        in_specs=[
            specs["scalars"],
            specs["scalars"],
            wide_block,
            wide_block,
            wide_block,
            specs["rate"],
            pl.BlockSpec((ROWS_STEP, states, SUBS, LANES), lambda i: (steps - 1 - i, 0, 0, 0)),
        ],
        out_specs=(wide_block, wide_block, pair_block, pair_block, specs["rate"]),
        scratch_shapes=[row_buffer] * 5
        + [
            pltpu.VMEM((ROWS_STEP * states * 8, LANES), jnp.float32),
            pltpu.VMEM((ROWS_STEP * states * 8, LANES), jnp.float32),
            pltpu.VMEM((states, SUBS, LANES), jnp.float32),
        ],
        cost_estimate=pl.CostEstimate(
            flops=18 * rows * states * width,
            transcendentals=rows * states * width,
            bytes_accessed=4 * rows * width * (states + 5),
        ),
    )(
        b_rows,
        c_rows,
        widen(steps_dt),
        widen(inputs),
        widen(d_out),
        widen(rates).reshape(states, SUBS, LANES),
        past,
    )
    return (
        d_dt[:, :inner],
        d_in[:, :inner],
        jnp.sum(d_b.reshape(rows, states, LANES), axis=-1),
        jnp.sum(d_c.reshape(rows, states, LANES), axis=-1),
        d_rate.reshape(states, width)[:, :inner],
    )


@jax.custom_vjp
def selective_scan(steps_dt, inputs, b_rows, c_rows, decay_log):
    return scan_forward(steps_dt, inputs, b_rows, c_rows, -jnp.exp(decay_log))[0]


def selective_scan_fwd(steps_dt, inputs, b_rows, c_rows, decay_log):
    rates = -jnp.exp(decay_log)
    out, past = scan_forward(steps_dt, inputs, b_rows, c_rows, rates)
    return out, (steps_dt, inputs, b_rows, c_rows, rates, past)


def selective_scan_bwd(kept, d_out):
    steps_dt, inputs, b_rows, c_rows, rates, past = kept
    d_dt, d_in, d_b, d_c, d_rate = scan_backward(
        steps_dt, inputs, b_rows, c_rows, rates, past, d_out
    )
    return d_dt, d_in, d_b, d_c, d_rate * rates


selective_scan.defvjp(selective_scan_fwd, selective_scan_bwd)


EPS = 1e-05
LEARN = 0.03
BETA_FIRST = 0.9
BETA_SECOND = 0.999
FIX_FIRST = 1.0 - 0.9**3
FIX_SECOND = 1.0 - 0.999**3
DECAY = 0.1
ADAM_EPS = 1e-08
NEGATIVE = -1e30


def matmul_f32(left, right):
    return jnp.dot(left, right, preferred_element_type=jnp.float32)


def batched(formula, left, right):
    return jnp.einsum(formula, left, right, preferred_element_type=jnp.float32)


def param_shapes():
    mixing = HEADS * HEAD + 2 * KVH * HEAD + 2 * INNER
    return [
        (D,),
        (D, mixing),
        (HEADS * HEAD, D),
        (CONV, INNER),
        (INNER,),
        (INNER, DTR + 2 * STATE),
        (DTR, INNER),
        (INNER,),
        (STATE, INNER),
        (INNER,),
        (INNER, D),
        (D,),
        (D,),
        (D,),
        (D, 2 * FF),
        (FF, D),
    ]


def unpack(flat_params):
    pieces = []
    cursor = 0
    for layout_shape in param_shapes():
        amount = math.prod(layout_shape)
        pieces.append(flat_params[cursor : cursor + amount].reshape(layout_shape))
        cursor += amount
    return pieces


def rms_norm(values, scale_gain):
    return values * lax.rsqrt(jnp.mean(values * values, axis=-1, keepdims=True) + EPS) * scale_gain


def token_layout(lengths, row_total):
    seq_slots = lengths.shape[0]
    blocks_used = (lengths + BLOCK - 1) // BLOCK
    firsts = jnp.cumsum(blocks_used) - blocks_used
    block_ids = jnp.arange(seq_slots, dtype=jnp.int32)
    inside = (
        (block_ids[:, None] >= firsts[None, :])
        & (block_ids[:, None] < (firsts + blocks_used)[None, :])
    ).astype(jnp.int32)
    occupied = jnp.sum(inside, axis=1) > 0
    block_segment = jnp.where(
        occupied, jnp.sum(inside * block_ids[None, :], axis=1), seq_slots + block_ids
    )
    block_begin = jnp.where(occupied, jnp.sum(inside * firsts[None, :], axis=1), block_ids)
    block_length = jnp.sum(inside * lengths[None, :], axis=1)
    rows_index = jnp.arange(row_total, dtype=jnp.int32)
    owner_block = (rows_index[:, None] // BLOCK == block_ids[None, :]).astype(jnp.int32)
    segment = jnp.sum(owner_block * block_segment[None, :], axis=1)
    places = rows_index - BLOCK * jnp.sum(owner_block * block_begin[None, :], axis=1)
    live_rows = places < jnp.sum(owner_block * block_length[None, :], axis=1)
    return (segment, places, live_rows)


def conv_silu(inner_in, conv_weight, conv_bias, places):
    summed = conv_bias + conv_weight[CONV - 1] * inner_in
    for offset in range(1, CONV):
        shifted = jnp.concatenate(
            [jnp.zeros((offset, inner_in.shape[1]), inner_in.dtype), inner_in[:-offset]], axis=0
        )
        summed = summed + conv_weight[CONV - 1 - offset] * jnp.where(
            (places >= offset)[:, None], shifted, jnp.zeros_like(shifted)
        )
    return jax.nn.silu(summed)


def mamba_tail(dt_raw, dt_bias, inputs, b_rows, c_rows, decay_log, skip, z_gate):
    steps_dt = jax.nn.softplus(dt_raw + dt_bias)
    scanned = selective_scan(steps_dt, inputs, b_rows, c_rows, decay_log)
    return (scanned + skip * inputs) * jax.nn.silu(z_gate)


def merge_branches(attn_out, ssm_out, beta_attn, beta_ssm):
    return 0.5 * (rms_norm(attn_out, beta_attn) + rms_norm(ssm_out, beta_ssm))


def swiglu(gate_up):
    return jax.nn.silu(gate_up[:, :FF]) * gate_up[:, FF:]


def attention_scores(query_rows, key_rows, allowed):
    row_total = query_rows.shape[0]
    query_heads = query_rows.reshape(row_total, KVH, HEADS // KVH, HEAD)
    key_heads = key_rows.reshape(row_total, KVH, HEAD)
    scores = batched("qkgd,pkd->kgqp", query_heads, key_heads) * HEAD ** (-0.5)
    return jnp.where(allowed, scores, NEGATIVE)


def attend_back(query_rows, key_rows, value_rows, soft_probs, d_heads):
    row_total = query_rows.shape[0]
    group_size = HEADS // KVH
    query_heads = query_rows.reshape(row_total, KVH, group_size, HEAD)
    key_heads = key_rows.reshape(row_total, KVH, HEAD)
    value_heads = value_rows.reshape(row_total, KVH, HEAD)
    probs_low = soft_probs.astype(jnp.bfloat16)
    d_heads4 = d_heads.reshape(row_total, KVH, group_size, HEAD)
    d_values = batched("kgqp,qkgd->pkd", probs_low, d_heads4)
    d_probs = batched("qkgd,pkd->kgqp", d_heads4, value_heads)
    centre = jnp.sum(soft_probs * d_probs, axis=-1, keepdims=True)
    d_scores = (soft_probs * (d_probs - centre) * HEAD ** (-0.5)).astype(jnp.bfloat16)
    d_query = batched("kgqp,pkd->qkgd", d_scores, key_heads)
    d_keys = batched("kgqp,qkgd->pkd", d_scores, query_heads)
    return (
        d_query.reshape(row_total, HEADS * HEAD),
        d_keys.reshape(row_total, KVH * HEAD),
        d_values.reshape(row_total, KVH * HEAD),
    )


def layer_pass(params, tokens, cotangent, lengths):
    (
        gain_in,
        w_mixing,
        w_attn,
        conv_weight,
        conv_bias,
        w_project,
        w_dt,
        dt_bias,
        decay_log,
        skip,
        w_ssm,
        beta_attn,
        beta_ssm,
        gain_ffn,
        w_gate_up,
        w_down,
    ) = unpack(params)
    wide = jnp.float32
    row_total = tokens.shape[0]
    segment, places, live_rows = token_layout(lengths, row_total)
    allowed = (segment[:, None] == segment[None, :]) & (places[None, :] <= places[:, None])
    residual = tokens.astype(wide)
    normed, norm_back = jax.vjp(rms_norm, residual, gain_in.astype(wide))
    normed_low = normed.astype(jnp.bfloat16)
    mixing = matmul_f32(normed_low, w_mixing)
    width_q = HEADS * HEAD
    width_kv = KVH * HEAD
    query_rows = mixing[:, :width_q].astype(jnp.bfloat16)
    key_rows = mixing[:, width_q : width_q + width_kv].astype(jnp.bfloat16)
    value_rows = mixing[:, width_q + width_kv : width_q + 2 * width_kv].astype(jnp.bfloat16)
    inner_in = mixing[:, width_q + 2 * width_kv : width_q + 2 * width_kv + INNER]
    z_gate = mixing[:, width_q + 2 * width_kv + INNER :]
    scores = attention_scores(query_rows, key_rows, allowed)
    row_max = jnp.max(scores, axis=-1, keepdims=True)
    logsum = row_max + jnp.log(jnp.sum(jnp.exp(scores - row_max), axis=-1, keepdims=True))
    forward_probs = jnp.exp(scores - logsum)
    probs_low = forward_probs.astype(jnp.bfloat16)
    value_heads = value_rows.reshape(row_total, KVH, HEAD)
    heads_out = (
        batched("kgqp,pkd->qkgd", probs_low, value_heads)
        .reshape(row_total, width_q)
        .astype(jnp.bfloat16)
    )
    attn_out = matmul_f32(heads_out, w_attn)
    activated, conv_back = jax.vjp(
        partial(conv_silu, places=places),
        inner_in,
        conv_weight.astype(wide),
        conv_bias.astype(wide),
    )
    activated_low = activated.astype(jnp.bfloat16)
    projected = matmul_f32(activated_low, w_project)
    dt_low = projected[:, :DTR].astype(jnp.bfloat16)
    b_rows = projected[:, DTR : DTR + STATE]
    c_rows = projected[:, DTR + STATE :]
    dt_raw = matmul_f32(dt_low, w_dt)
    activated_wide = lax.optimization_barrier(activated_low).astype(wide)
    gated_out, tail_back = jax.vjp(
        mamba_tail,
        dt_raw,
        dt_bias.astype(wide),
        activated_wide,
        b_rows,
        c_rows,
        decay_log.astype(wide),
        skip.astype(wide),
        z_gate,
    )
    gated_low = gated_out.astype(jnp.bfloat16)
    ssm_out = matmul_f32(gated_low, w_ssm)
    branch_mix, merge_back = jax.vjp(
        merge_branches, attn_out, ssm_out, beta_attn.astype(wide), beta_ssm.astype(wide)
    )
    hidden = residual + branch_mix
    normed_ffn, ffn_norm_back = jax.vjp(rms_norm, hidden, gain_ffn.astype(wide))
    normed_ffn_low = normed_ffn.astype(jnp.bfloat16)
    gate_up = matmul_f32(normed_ffn_low, w_gate_up)
    swished, swiglu_back = jax.vjp(swiglu, gate_up)
    swished_low = swished.astype(jnp.bfloat16)
    output = hidden + matmul_f32(swished_low, w_down)
    d_out = jnp.where(live_rows[:, None], cotangent, jnp.zeros_like(cotangent))
    grad_down = matmul_f32(swished_low.T, d_out)
    (d_gate_up,) = swiglu_back(matmul_f32(d_out, w_down.T))
    d_gate_up_low = d_gate_up.astype(jnp.bfloat16)
    grad_gate_up = matmul_f32(normed_ffn_low.T, d_gate_up_low)
    d_hidden, grad_gain_ffn = ffn_norm_back(matmul_f32(d_gate_up_low, w_gate_up.T))
    d_hidden = d_hidden + d_out.astype(wide)
    d_attn, d_ssm, grad_beta_attn, grad_beta_ssm = merge_back(d_hidden)
    d_ssm_low = d_ssm.astype(jnp.bfloat16)
    grad_ssm = matmul_f32(gated_low.T, d_ssm_low)
    d_dt_raw, grad_dt_bias, d_activated, d_b_rows, d_c_rows, grad_decay, grad_skip, d_z_gate = (
        tail_back(matmul_f32(d_ssm_low, w_ssm.T))
    )
    d_dt_low = d_dt_raw.astype(jnp.bfloat16)
    grad_dt = matmul_f32(dt_low.T, d_dt_low)
    d_projected = jnp.concatenate(
        [matmul_f32(d_dt_low, w_dt.T), d_b_rows, d_c_rows], axis=1
    ).astype(jnp.bfloat16)
    grad_project = matmul_f32(activated_low.T, d_projected)
    d_activated = d_activated + matmul_f32(d_projected, w_project.T)
    d_inner_in, grad_conv_weight, grad_conv_bias = conv_back(d_activated)
    d_attn_low = d_attn.astype(jnp.bfloat16)
    grad_attn = matmul_f32(heads_out.T, d_attn_low)
    d_heads = matmul_f32(d_attn_low, w_attn.T).astype(jnp.bfloat16)
    soft_probs = jnp.exp(attention_scores(query_rows, key_rows, allowed) - logsum)
    d_query, d_keys, d_values = attend_back(query_rows, key_rows, value_rows, soft_probs, d_heads)
    d_mixing = jnp.concatenate([d_query, d_keys, d_values, d_inner_in, d_z_gate], axis=1).astype(
        jnp.bfloat16
    )
    grad_mixing = matmul_f32(normed_low.T, d_mixing)
    d_residual, grad_gain_in = norm_back(matmul_f32(d_mixing, w_mixing.T))
    d_tokens = d_hidden + d_residual
    gradients = [
        grad_gain_in,
        grad_mixing,
        grad_attn,
        grad_conv_weight,
        grad_conv_bias,
        grad_project,
        grad_dt,
        grad_dt_bias,
        grad_decay,
        grad_skip,
        grad_ssm,
        grad_beta_attn,
        grad_beta_ssm,
        grad_gain_ffn,
        grad_gate_up,
        grad_down,
    ]
    flat_grad = jnp.concatenate(
        [member.astype(jnp.bfloat16).reshape(-1) for member in gradients]
        + [jnp.zeros((params.shape[0] - PARAMS,), jnp.bfloat16)]
    )
    live_count = jnp.sum(live_rows.astype(wide))
    return (output.astype(jnp.bfloat16), d_tokens, flat_grad, live_count)


def adamw_update(weight, gradient, first_moment, second):
    first_moment = BETA_FIRST * first_moment + (1.0 - BETA_FIRST) * gradient
    second = BETA_SECOND * second + (1.0 - BETA_SECOND) * gradient * gradient
    step_size = first_moment / FIX_FIRST / (jnp.sqrt(second / FIX_SECOND) + ADAM_EPS)
    return (weight - LEARN * (step_size + DECAY * weight), first_moment, second)


def local(tokens, cotangent, lengths, master, moment_first, moment_second):
    group_count = lax.axis_size("dp")
    piece = master.shape[0] // group_count
    mine = lax.dynamic_slice(master, (lax.axis_index("dp") * piece,), (piece,))
    weights = lax.all_gather(mine.astype(jnp.bfloat16), ("shard", "dp"), axis=0, tiled=True)
    output, d_tokens, flat_grad, live_count = layer_pass(weights, tokens, cotangent, lengths[0])
    piece_sum = lax.psum_scatter(flat_grad, ("shard", "dp"), scatter_dimension=0, tiled=True)
    owned_sum = lax.all_gather(piece_sum, "dp", axis=0, tiled=True).astype(jnp.float32)
    total = lax.psum(live_count, ("dp", "shard"))
    gradient = owned_sum / total
    new_master, new_first, new_second = adamw_update(master, gradient, moment_first, moment_second)
    return (output, d_tokens.astype(jnp.bfloat16), gradient, new_master, new_first, new_second)


def solution(mesh):
    return jax.shard_map(
        local,
        mesh=mesh,
        in_specs=(
            P(("dp", "shard"), None),
            P(("dp", "shard"), None),
            P(("dp", "shard"), None),
            P("shard"),
            P("shard"),
            P("shard"),
        ),
        out_specs=(
            P(("dp", "shard"), None),
            P(("dp", "shard"), None),
            P("shard"),
            P("shard"),
            P("shard"),
            P("shard"),
        ),
        check_vma=False,
    )
```
